256 devices in a mesh: trial: 4 (over x), fsdp: 16 (over z, core), cols: 4 (over y).
Axes of the slice: x: 4, y: 4, z: 8, core: 2. Of those that a mesh axis runs over, the one named last changes fastest.
Arguments:
- train_gate: bfloat16 [8192, 8192], P(('trial', 'fsdp'), 'cols'), parts along dimension 0, may hold values from -0.1875 to 0.1875
- low_gate: bfloat16 [8192, 16], P(('trial', 'fsdp')), parts along dimension 0, may hold values from -0.125 to 0.125
- high_gate: bfloat16 [64, 8192], P('trial', 'cols'), parts along dimension 0, may hold values from -1.5 to 1.5
- train_up: bfloat16 [8192, 8192], P(('trial', 'fsdp'), 'cols'), parts along dimension 0, may hold values from -0.1875 to 0.1875
- low_up: bfloat16 [8192, 16], P(('trial', 'fsdp')), parts along dimension 0, may hold values from -0.125 to 0.125
- high_up: bfloat16 [64, 8192], P('trial', 'cols'), parts along dimension 0, may hold values from -1.5 to 1.5
- norm_gain: float32 [8192], P(('trial', 'fsdp')), parts along dimension 0, may hold values from 0.25 to 1.75
Outputs:
- ready_gate: bfloat16 [8192, 8192], P('trial', 'cols'), parts along dimension 0
- ready_up: bfloat16 [8192, 8192], P('trial', 'cols'), parts along dimension 0
- column_gate: float32 [32768], P(('trial', 'cols')), parts along dimension 0
- column_up: float32 [32768], P(('trial', 'cols')), parts along dimension 0
The draws below stay inside these ranges and needn't reach their ends.
There are 4 independent parts, one for each index of `trial`. The reference program is written for one: setup_inputs(seed, part) draws one part's arguments, and reference() takes and returns one part's arrays. A program takes and returns all parts, laid end to end along the dimension named above; each array names one. Nothing has to cross between parts.
All inputs are finite; a program needn't handle non-finite values. Where the reference program divides by a largest or mean magnitude, that divisor is 1e-20 or more.
Results may differ from the reference program's by a relative error of at most 0.001.
Values may be sent and summed in bfloat16 or wider, within the bound.
A program may use at most 128 MiB of HBM per device.

```python
import jax
import jax.numpy as jnp

D_MODEL = 2048
D_INNER = 8192
RANK = 16


def spiked(drawn, own_key, source, target, shards_of, factor):
    owner, partner = [(jnp.arange(drawn.shape[axis_at]) // (drawn.shape[axis_at] // shards_of)).reshape([-1 if axis == axis_at else 1 for axis in range(drawn.ndim)]) for axis_at in (source, target)]
    chosen = jax.random.permutation(own_key, shards_of)[partner]
    strong = (owner == chosen) | (owner == (partner + shards_of // 2) % shards_of)
    return jnp.where(strong, factor * drawn, drawn)


def levels(key, shape, split, least, high):
    def one(dim, parts):
        draws = jax.random.uniform(jax.random.fold_in(jax.random.fold_in(key, 6), dim), (parts,), jnp.float32, least / len(split), high / len(split))
        return jnp.repeat(jnp.exp(draws), shape[dim] // parts).reshape((-1,) + (1,) * (len(shape) - dim - 1))

    factor_of = one(*split[0])
    for cut in split[1:]:
        factor_of = factor_of * one(*cut)
    return factor_of


def gaussian(own_key, shape, spread, bound, shards=(), held_as=jnp.bfloat16):
    drawn = jax.random.normal(own_key, shape, jnp.float32) * spread
    if len(shards) > 0:
        drawn = levels(own_key, shape, shards, -0.22, 0.18) * drawn
    return jnp.clip(drawn, min=-bound, max=bound).astype(held_as)


def gaussian_with(stream_key, shape, spread, bound, split, heavy, kind=jnp.bfloat16):
    array = spread * jax.random.normal(stream_key, shape, jnp.float32)
    if split:
        array = array * levels(stream_key, shape, split, -0.22, 0.18)
    return jnp.clip(spiked(array, jax.random.fold_in(stream_key, 3), *heavy), -bound, bound).astype(kind)


def setup_inputs(seed: int = 0, part: int = 0) -> dict:
    seeds = jax.random.split(jax.random.key(seed), 8)
    own_keys = jax.random.split(jax.random.fold_in(seeds[7], part), 8)
    train_gate = gaussian_with(own_keys[0], (D_MODEL, D_INNER), D_MODEL ** -0.5, 0.1875, ((0, 16), (1, 4)), (0, 1, 16, 2.0))
    low_gate = gaussian(own_keys[1], (D_MODEL, RANK), D_MODEL ** -0.5, 0.125, ((0, 16),))
    high_gate = gaussian(own_keys[2], (RANK, D_INNER), RANK ** -0.5, 1.5, ((1, 4),))
    train_up = gaussian_with(own_keys[3], (D_MODEL, D_INNER), D_MODEL ** -0.5, 0.1875, ((0, 16), (1, 4)), (0, 1, 16, 2.0))
    low_up = gaussian(own_keys[4], (D_MODEL, RANK), D_MODEL ** -0.5, 0.125, ((0, 16),))
    high_up = gaussian(own_keys[5], (RANK, D_INNER), RANK ** -0.5, 1.5, ((1, 4),))
    norm_gain = jnp.clip(1.0 + 0.15 * jax.random.normal(own_keys[6], (D_MODEL,), jnp.float32), 0.25, 1.75)
    return {"train_gate": train_gate, "low_gate": low_gate, "high_gate": high_gate, "train_up": train_up, "low_up": low_up, "high_up": high_up, "norm_gain": norm_gain}


mix_rate = 1.0


def reference(train_gate, low_gate, high_gate, train_up, low_up, high_up, norm_gain):
    latest_gate = train_gate.astype(jnp.float32) + mix_rate * jnp.dot(low_gate, high_gate, preferred_element_type=jnp.float32)
    latest_up = train_up.astype(jnp.float32) + mix_rate * jnp.dot(low_up, high_up, preferred_element_type=jnp.float32)
    latest_gained_gate = latest_gate * norm_gain[:, None]
    latest_gained_up = latest_up * norm_gain[:, None]
    column_gate = jnp.max(jnp.abs(latest_gained_gate), axis=0)
    ready_gate = (latest_gained_gate / column_gate).astype(jnp.bfloat16)
    column_up = jnp.max(jnp.abs(latest_gained_up), axis=0)
    ready_up = (latest_gained_up / column_up).astype(jnp.bfloat16)
    return ready_gate, ready_up, column_gate, column_up
```

```python
import functools

import jax
import jax.numpy as jnp
from jax import lax
from jax.experimental import pallas as pl
from jax.experimental.pallas import tpu as pltpu
from jax.sharding import PartitionSpec as P

MESH = pl.DeviceIdType.MESH
BF16, F32 = jnp.bfloat16, jnp.float32

N = 16
ROWS = 128
COLS = 2048
RANK = 16
NCB = 8
W = COLS // NCB
GROUP = 4
SIDE = 56


def gather(
    tg, lg, hg, tu, lu, hu, gn,
    out, cmax,
    raw, side, gain, high, low, gainb, part,
    load_sem, side_sem, ring_recv, ring_send, side_send, pair_recv, pair_send, own_recv, own_send,
):
    trial, me, cols = lax.axis_index("trial"), lax.axis_index("fsdp"), lax.axis_index("cols")
    right, left = lax.rem(me + 2, N), lax.rem(me + N - 2, N)
    pair = me + 1 - 2 * lax.rem(me, 2)
    ahead = (right, left)

    def to(f):
        return (trial, f, cols)

    def source(f, way, hops):
        return lax.rem(f + N - 2 * hops, N) if way == 0 else lax.rem(f + 2 * hops, N)

    loads = []
    for p, (low_in, high_in) in enumerate(((lg, hg), (lu, hu))):
        loads.append(pltpu.make_async_copy(low_in, side.at[me, pl.ds(p * RANK, RANK)], side_sem.at[p]))
        loads.append(pltpu.make_async_copy(high_in, high.at[p], side_sem.at[2 + p]))
    loads.append(pltpu.make_async_copy(gn, gain.at[me], side_sem.at[4]))

    def own_load(p, cb):
        train = (tg, tu)[p]
        return pltpu.make_async_copy(
            train.at[:, pl.ds(pl.multiple_of(cb * W, W), W)], raw.at[p, me, cb], load_sem.at[p, cb]
        )

    for copy in loads:
        copy.start()
    for cb in range(NCB):
        for p in range(2):
            own_load(p, cb).start()

    barrier = pltpu.get_barrier_semaphore()
    for f in (right, left, pair):
        pl.semaphore_signal(barrier, inc=1, device_id=to(f), device_id_type=MESH)
    pl.semaphore_wait(barrier, 3)

    def remote(ref, send, recv, f):
        return pltpu.make_async_remote_copy(
            src_ref=ref, dst_ref=ref, send_sem=send, recv_sem=recv, device_id=to(f), device_id_type=MESH
        )

    def chunk_at(hops, cb, short):
        return (hops - 1) * 2 * NCB + cb * 2 + short

    def ring_chunk(way, p, src, cb, at):
        return remote(raw.at[p, src, cb], ring_send.at[way], ring_recv.at[way, at], ahead[way])

    def pair_chunk(way, p, src, cb, at):
        return remote(raw.at[p, src, cb], pair_send, pair_recv.at[way, at], pair)

    def own_chunk(p, src, cb):
        return remote(raw.at[p, src, cb], pair_send, own_recv.at[p * NCB + cb], pair)

    def side_ref(way, src, hops):
        return side.at[src, pl.ds(way * RANK, RANK)] if hops == 4 else side.at[src]

    def ring_side(way, src, hops):
        copies = [remote(side_ref(way, src, hops), side_send.at[way, hops - 1], ring_recv.at[way, SIDE + hops - 1], ahead[way])]
        if way == 0 or hops < 4:
            copies.append(remote(gain.at[src], side_send.at[way, 3 + hops], ring_recv.at[way, SIDE + 3 + hops], ahead[way]))
        return copies

    def pair_side(way, src, hops):
        copies = [remote(side_ref(way, src, hops), own_send.at[way, hops - 1], pair_recv.at[way, SIDE + hops - 1], pair)]
        if way == 0 or hops < 4:
            copies.append(remote(gain.at[src], own_send.at[way, 3 + hops], pair_recv.at[way, SIDE + 3 + hops], pair))
        return copies

    def own_side(src):
        return [
            remote(side.at[src], own_send.at[0, 8], own_recv.at[2 * NCB], pair),
            remote(gain.at[src], own_send.at[1, 8], own_recv.at[2 * NCB + 1], pair),
        ]

    for copy in loads:
        copy.wait()
    for way in range(2):
        for copy in ring_side(way, me, 1):
            copy.start()
    for copy in own_side(me):
        copy.start()

    def send_own(cb, _):
        for p in range(2):
            own_load(p, cb).wait()
        for k in range(2):
            for way in range(2):
                p = way if k == 0 else 1 - way
                ring_chunk(way, p, me, cb, chunk_at(1, cb, k)).start()
        for p in range(2):
            own_chunk(p, me, cb).start()
        return 0

    lax.fori_loop(0, NCB, send_own, 0)

    def rows(src, n=1):
        return pl.ds(pl.multiple_of(src * ROWS, ROWS), n * ROWS)

    def prepare(src):
        for p in range(2):
            low[p, rows(src), :] = side[src, pl.ds(p * RANK, RANK), :].astype(F32).T.astype(BF16)
        gainb[rows(src), :] = jnp.broadcast_to(gain[src], (ROWS, ROWS)).T

    def merged(p, src, cb, n):
        train = raw[p, pl.ds(src, n), cb].reshape(n * ROWS, W).astype(F32)
        delta = jnp.dot(
            low[p, rows(src, n), :],
            high[p, :, pl.ds(pl.multiple_of(cb * W, W), W)],
            preferred_element_type=F32,
        )
        scale = gainb[rows(src, n), :]
        return (train + delta) * jnp.concatenate([scale] * (W // ROWS), axis=1)

    def note(p, src, cb):
        size = jnp.abs(merged(p, src, cb, 1)).reshape(ROWS // 8, 8, W).max(axis=0)
        part[p, cb] = jnp.maximum(part[p, cb], size)

    part[...] = jnp.zeros_like(part)
    prepare(me)

    def note_own(cb, _):
        for p in range(2):
            note(p, me, cb)
        return 0

    lax.fori_loop(0, NCB, note_own, 0)

    for copy in own_side(pair):
        copy.wait_recv()
    prepare(pair)

    def note_pair(cb, _):
        for p in range(2):
            own_chunk(p, pair, cb).wait_recv()
            note(p, pair, cb)
        return 0

    lax.fori_loop(0, NCB, note_pair, 0)

    for hops in (1, 2, 3):
        for way in range(2):
            src = source(me, way, hops)
            for copy in ring_side(way, src, hops):
                copy.wait_recv()
            for copy in ring_side(way, src, hops + 1) + pair_side(way, src, hops):
                copy.start()
            prepare(src)
        for way in range(2):
            src = source(pair, way, hops)
            for copy in pair_side(way, src, hops):
                copy.wait_recv()
            prepare(src)

        def step(cb, _, hops=hops):
            for k in range(2):
                for way in range(2):
                    p, src = (way if k == 0 else 1 - way), source(me, way, hops)
                    at = chunk_at(hops, cb, k)
                    ring_chunk(way, p, src, cb, at).wait_recv()
                    if hops < 3:
                        ring_chunk(way, p, src, cb, chunk_at(hops + 1, cb, k)).start()
                    elif k == 0:
                        ring_chunk(way, p, src, cb, 6 * NCB + cb).start()
                    pair_chunk(way, p, src, cb, at).start()
            for k in range(2):
                for way in range(2):
                    note(way if k == 0 else 1 - way, source(me, way, hops), cb)
            for k in range(2):
                for way in range(2):
                    p, src = (way if k == 0 else 1 - way), source(pair, way, hops)
                    pair_chunk(way, p, src, cb, chunk_at(hops, cb, k)).wait_recv()
                    note(p, src, cb)
            return 0

        lax.fori_loop(0, NCB, step, 0)

    far, far_pair = source(me, 0, 4), source(pair, 0, 4)
    for way in range(2):
        for copy in ring_side(way, far, 4):
            copy.wait_recv()
        for copy in pair_side(way, far, 4):
            copy.start()
    prepare(far)
    for way in range(2):
        for copy in pair_side(way, far_pair, 4):
            copy.wait_recv()
    prepare(far_pair)

    def finish(cb):
        for p in range(2):
            pair_chunk(p, p, far_pair, cb, 6 * NCB + cb).wait_recv()
            note(p, far_pair, cb)
        for p in range(2):
            largest = part[p, cb].max(axis=0, keepdims=True)
            cmax[p, :, pl.ds(pl.multiple_of(cb * W, W), W)] = largest
            part[p, cb] = jnp.broadcast_to(1.0 / largest, (8, W))

        def scale(i, _):
            for p in range(2):
                whole = merged(p, i * GROUP, cb, GROUP) * part[p, cb, :1]
                out[p, rows(i * GROUP, GROUP), pl.ds(pl.multiple_of(cb * W, W), W)] = whole.astype(BF16)
            return 0

        lax.fori_loop(0, N // GROUP, scale, 0)

    def last(cb, _):
        for p in range(2):
            ring_chunk(p, p, far, cb, 6 * NCB + cb).wait_recv()
            pair_chunk(p, p, far, cb, 6 * NCB + cb).start()
        for p in range(2):
            note(p, far, cb)

        @pl.when(cb > 0)
        def _():
            finish(cb - 1)

        return 0

    lax.fori_loop(0, NCB, last, 0)
    finish(NCB - 1)

    for way in range(2):
        sent = raw.at[0, pl.ds(0, 7)]
        pltpu.make_async_copy(sent, sent, ring_send.at[way]).wait()
        for hops in (1, 2, 3, 4):
            src = source(me, way, hops - 1)
            for copy in ring_side(way, src, hops):
                copy.wait_send()
            for copy in pair_side(way, source(me, way, hops), hops):
                copy.wait_send()
    for copy in own_side(me):
        copy.wait_send()
    pltpu.make_async_copy(raw.at[0], raw.at[0], pair_send).wait()


PIECES = 8


def write(new, cmax, gate, up, col_gate, col_up, sem):
    copies = []
    for p, (dst, col) in enumerate(((gate, col_gate), (up, col_up))):
        for i in range(PIECES):
            at = pl.ds(i * (COLS // PIECES), COLS // PIECES)
            copies.append(pltpu.make_async_copy(new.at[p, at], dst.at[at], sem.at[p, i]))
        copies.append(pltpu.make_async_copy(cmax.at[p], col, sem.at[p, PIECES]))
    for copy in copies:
        copy.start()
    for copy in copies:
        copy.wait()


def per_device(train_gate, low_gate, high_gate, train_up, low_up, high_up, norm_gain):
    anywhere = pl.BlockSpec(memory_space=pl.ANY)
    vmem = pl.BlockSpec(memory_space=pltpu.VMEM)
    dma = pltpu.SemaphoreType.DMA
    new, cmax = pl.pallas_call(
        gather,
        name="gather",
        out_shape=(pltpu.VMEM((2, N * ROWS, COLS), BF16), pltpu.VMEM((2, 1, COLS), F32)),
        in_specs=[anywhere] * 7,
        out_specs=(vmem, vmem),
        scratch_shapes=[
            pltpu.VMEM((2, N, NCB, ROWS, W), BF16),
            pltpu.VMEM((N, 2 * RANK, ROWS), BF16),
            pltpu.VMEM((N, 1, ROWS), F32),
            pltpu.VMEM((2, RANK, COLS), BF16),
            pltpu.VMEM((2, N * ROWS, RANK), BF16),
            pltpu.VMEM((N * ROWS, ROWS), F32),
            pltpu.VMEM((2, NCB, 8, W), F32),
            dma((2, NCB)),
            dma((5,)),
            dma((2, SIDE + 8)),
            dma((2,)),
            dma((2, 8)),
            dma((2, SIDE + 8)),
            dma,
            dma((2 * NCB + 2,)),
            dma((2, 9)),
        ],
        compiler_params=pltpu.CompilerParams(
            collective_id=0, has_side_effects=True, vmem_limit_bytes=40 * 2**20
        ),
    )(train_gate, low_gate.T, high_gate, train_up, low_up.T, high_up, norm_gain.reshape(1, ROWS))
    hbm = pl.BlockSpec(memory_space=pltpu.HBM)
    gate, up, col_gate, col_up = pl.pallas_call(
        write,
        name="write",
        out_shape=(
            jax.ShapeDtypeStruct((N * ROWS, COLS), BF16),
            jax.ShapeDtypeStruct((N * ROWS, COLS), BF16),
            jax.ShapeDtypeStruct((1, COLS), F32),
            jax.ShapeDtypeStruct((1, COLS), F32),
        ),
        in_specs=[vmem, vmem],
        out_specs=(hbm,) * 4,
        scratch_shapes=[dma((2, PIECES + 1))],
        compiler_params=pltpu.CompilerParams(vmem_limit_bytes=20 * 2**20),
    )(new, cmax)
    return gate, up, col_gate.reshape(COLS), col_up.reshape(COLS)


def solution(mesh):
    placed = (
        P(("trial", "fsdp"), "cols"),
        P(("trial", "fsdp"), None),
        P("trial", "cols"),
        P(("trial", "fsdp"), "cols"),
        P(("trial", "fsdp"), None),
        P("trial", "cols"),
        P(("trial", "fsdp")),
    )
    return jax.shard_map(
        per_device,
        mesh=mesh,
        in_specs=placed,
        out_specs=(
            P("trial", "cols"),
            P("trial", "cols"),
            P(("trial", "cols")),
            P(("trial", "cols")),
        ),
        check_vma=False,
    )
```

```python
import functools

import jax
import jax.numpy as jnp
from jax import lax
from jax.experimental import pallas as pl
from jax.experimental.pallas import tpu as pltpu
from jax.sharding import PartitionSpec as P

MESH = pl.DeviceIdType.MESH
BF16, F32 = jnp.bfloat16, jnp.float32

N = 16
ROWS = 128
COLS = 2048
RANK = 16
NCB = 4
W = COLS // NCB
GROUP = 2
SIDE = 28


def rows(src, n=1):
    return pl.ds(pl.multiple_of(src * ROWS, ROWS), n * ROWS)


def columns(cb):
    return pl.ds(pl.multiple_of(cb * W, W), W)


def merged_weights(raw, high, low, gainb, p, src, cb, n):
    train = raw[p, pl.ds(src, n), cb].reshape(n * ROWS, W).astype(F32)
    delta = jnp.dot(low[p, rows(src, n), :], high[p, :, columns(cb)], preferred_element_type=F32)
    scale = gainb[rows(src, n), :]
    return (train + delta) * jnp.concatenate([scale] * (W // ROWS), axis=1)


def gather(
    tg, lg, hg, tu, lu, hu, gn,
    out, cmax, raw, high, low, gainb, part,
    side, gain,
    load_sem, side_sem, ring_recv, ring_send, side_send, pair_recv, pair_send, own_recv, own_send,
):
    trial, me, cols = lax.axis_index("trial"), lax.axis_index("fsdp"), lax.axis_index("cols")
    right, left = lax.rem(me + 2, N), lax.rem(me + N - 2, N)
    pair = me + 1 - 2 * lax.rem(me, 2)
    ahead = (right, left)

    def to(f):
        return (trial, f, cols)

    def source(f, way, hops):
        return lax.rem(f + N - 2 * hops, N) if way == 0 else lax.rem(f + 2 * hops, N)

    loads = []
    for p, (low_in, high_in) in enumerate(((lg, hg), (lu, hu))):
        loads.append(pltpu.make_async_copy(low_in, side.at[me, pl.ds(p * RANK, RANK)], side_sem.at[p]))
        loads.append(pltpu.make_async_copy(high_in, high.at[p], side_sem.at[2 + p]))
    loads.append(pltpu.make_async_copy(gn, gain.at[me], side_sem.at[4]))

    def own_load(p, cb):
        train = (tg, tu)[p]
        return pltpu.make_async_copy(
            train.at[:, pl.ds(pl.multiple_of(cb * W, W), W)], raw.at[p, me, cb], load_sem.at[p, cb]
        )

    for copy in loads:
        copy.start()
    for cb in range(NCB):
        for p in range(2):
            own_load(p, cb).start()

    barrier = pltpu.get_barrier_semaphore()
    for f in (right, left, pair):
        pl.semaphore_signal(barrier, inc=1, device_id=to(f), device_id_type=MESH)
    pl.semaphore_wait(barrier, 3)

    def remote(ref, send, recv, f):
        return pltpu.make_async_remote_copy(
            src_ref=ref, dst_ref=ref, send_sem=send, recv_sem=recv, device_id=to(f), device_id_type=MESH
        )

    def chunk_at(hops, cb, short):
        return (hops - 1) * 2 * NCB + cb * 2 + short

    def ring_chunk(way, p, src, cb, at):
        return remote(raw.at[p, src, cb], ring_send.at[way], ring_recv.at[way, at], ahead[way])

    def pair_chunk(way, p, src, cb, at):
        return remote(raw.at[p, src, cb], pair_send, pair_recv.at[way, at], pair)

    def own_chunk(p, src, cb):
        return remote(raw.at[p, src, cb], pair_send, own_recv.at[p * NCB + cb], pair)

    def side_ref(way, src, hops):
        return side.at[src, pl.ds(way * RANK, RANK)] if hops == 4 else side.at[src]

    def ring_side(way, src, hops):
        copies = [remote(side_ref(way, src, hops), side_send.at[way, hops - 1], ring_recv.at[way, SIDE + hops - 1], ahead[way])]
        if way == 0 or hops < 4:
            copies.append(remote(gain.at[src], side_send.at[way, 3 + hops], ring_recv.at[way, SIDE + 3 + hops], ahead[way]))
        return copies

    def pair_side(way, src, hops):
        copies = [remote(side_ref(way, src, hops), own_send.at[way, hops - 1], pair_recv.at[way, SIDE + hops - 1], pair)]
        if way == 0 or hops < 4:
            copies.append(remote(gain.at[src], own_send.at[way, 3 + hops], pair_recv.at[way, SIDE + 3 + hops], pair))
        return copies

    def own_side(src):
        return [
            remote(side.at[src], own_send.at[0, 8], own_recv.at[2 * NCB], pair),
            remote(gain.at[src], own_send.at[1, 8], own_recv.at[2 * NCB + 1], pair),
        ]

    for copy in loads:
        copy.wait()
    for way in range(2):
        for copy in ring_side(way, me, 1):
            copy.start()
    for copy in own_side(me):
        copy.start()

    def send_own(cb, _):
        for p in range(2):
            own_load(p, cb).wait()
        for k in range(2):
            for way in range(2):
                p = way if k == 0 else 1 - way
                ring_chunk(way, p, me, cb, chunk_at(1, cb, k)).start()
        for p in range(2):
            own_chunk(p, me, cb).start()
        return 0

    lax.fori_loop(0, NCB, send_own, 0)

    def prepare(src):
        for p in range(2):
            low[p, rows(src), :] = side[src, pl.ds(p * RANK, RANK), :].astype(F32).T.astype(BF16)
        gainb[rows(src), :] = jnp.broadcast_to(gain[src], (ROWS, ROWS)).T

    merged = functools.partial(merged_weights, raw, high, low, gainb)

    def note(p, src, cb):
        size = jnp.abs(merged(p, src, cb, 1)).reshape(ROWS // 8, 8, W).max(axis=0)
        part[p, cb] = jnp.maximum(part[p, cb], size)

    part[...] = jnp.zeros_like(part)
    prepare(me)

    def note_own(cb, _):
        for p in range(2):
            note(p, me, cb)
        return 0

    lax.fori_loop(0, NCB, note_own, 0)

    for copy in own_side(pair):
        copy.wait_recv()
    prepare(pair)

    def note_pair(cb, _):
        for p in range(2):
            own_chunk(p, pair, cb).wait_recv()
            note(p, pair, cb)
        return 0

    lax.fori_loop(0, NCB, note_pair, 0)

    def pieces(f, hops):
        for k in range(2 if hops < 4 else 1):
            for way in range(2):
                yield way, (way if k == 0 else 1 - way), source(f, way, hops), k

    def at_hop(hops, cb, k):
        return chunk_at(hops, cb, k) if hops < 4 else 6 * NCB + cb

    def forward(hops, cb, ks=(0, 1)):
        for way, p, src, k in pieces(me, hops):
            if k in ks:
                ring_chunk(way, p, src, cb, at_hop(hops + 1, cb, k)).start()

    def receive(hops, cb, ks=(), relay=True):
        for way, p, src, k in pieces(me, hops):
            ring_chunk(way, p, src, cb, at_hop(hops, cb, k)).wait_recv()
            if k in ks:
                ring_chunk(way, p, src, cb, at_hop(hops + 1, cb, k)).start()
            pair_chunk(way, p, src, cb, at_hop(hops, cb, k)).start()

    def note_own_side(hops, cb):
        for way, p, src, k in pieces(me, hops):
            note(p, src, cb)

    def note_other_core(hops, cb):
        for way, p, src, k in pieces(pair, hops):
            pair_chunk(way, p, src, cb, at_hop(hops, cb, k)).wait_recv()
            note(p, src, cb)

    def sides(hops):
        for way in range(2):
            src = source(me, way, hops)
            for copy in ring_side(way, src, hops):
                copy.wait_recv()
            for copy in (ring_side(way, src, hops + 1) if hops < 4 else []) + pair_side(way, src, hops):
                copy.start()
            if hops < 4 or way == 1:
                prepare(src)
        for way in range(2):
            src = source(pair, way, hops)
            for copy in pair_side(way, src, hops):
                copy.wait_recv()
            if hops < 4 or way == 1:
                prepare(src)

    def scale(cb):
        for p in range(2):
            largest = part[p, cb].max(axis=0, keepdims=True)
            cmax[p, :, columns(cb)] = largest
            part[p, cb] = jnp.broadcast_to(1.0 / largest, (8, W))

        def group(i, _):
            for p in range(2):
                whole = merged(p, i * GROUP, cb, GROUP) * part[p, cb, :1]
                out[p, rows(i * GROUP, GROUP), columns(cb)] = whole.astype(BF16)
            return 0

        lax.fori_loop(0, N // GROUP, group, 0)

    sides(1)

    def step(cb, _):
        receive(1, cb, (0, 1))
        note_own_side(1, cb)
        note_other_core(1, cb)
        return 0

    lax.fori_loop(0, NCB, step, 0)

    sides(2)

    def step_2(cb, _):
        receive(2, cb)

        @pl.when(cb < 2)
        def _():
            forward(2, cb)

        note_own_side(2, cb)
        note_other_core(2, cb)
        return 0

    lax.fori_loop(0, NCB, step_2, 0)
    sides(3)
    sides_due = True
    for cb in range(NCB):
        receive(3, cb, (0,))
        if cb + 2 < NCB:
            forward(2, cb + 2)
        note_own_side(3, cb)
        if cb > 0:
            if sides_due:
                sides(4)
                sides_due = False
            receive(4, cb - 1)
            note_own_side(4, cb - 1)
            note_other_core(3, cb - 1)
            note_other_core(4, cb - 1)
            scale(cb - 1)
    receive(4, NCB - 1)
    note_own_side(4, NCB - 1)
    note_other_core(3, NCB - 1)
    note_other_core(4, NCB - 1)
    for p in range(2):
        largest = part[p, NCB - 1].max(axis=0, keepdims=True)
        cmax[p, :, columns(NCB - 1)] = largest
        part[p, NCB - 1] = jnp.broadcast_to(1.0 / largest, (8, W))

    for way in range(2):
        sent = raw.at[0, pl.ds(0, 7)]
        pltpu.make_async_copy(sent, sent, ring_send.at[way]).wait()
        for hops in (1, 2, 3, 4):
            src = source(me, way, hops - 1)
            for copy in ring_side(way, src, hops):
                copy.wait_send()
            for copy in pair_side(way, source(me, way, hops), hops):
                copy.wait_send()
    for copy in own_side(me):
        copy.wait_send()
    pltpu.make_async_copy(raw.at[0], raw.at[0], pair_send).wait()


PIECES = 8
DONE = (NCB - 1) * W


def write(new, cmax, raw, high, low, gainb, part, gate, up, col_gate, col_up, rest, sem, rest_sem):
    copies = []
    for i in range(PIECES):
        at = pl.ds(i * (N * ROWS // PIECES), N * ROWS // PIECES)
        for p, dst in enumerate((gate, up)):
            copies.append(pltpu.make_async_copy(new.at[p, at], dst.at[at, pl.ds(0, DONE)], sem.at[p, i]))
    for p, col in enumerate((col_gate, col_up)):
        copies.append(pltpu.make_async_copy(cmax.at[p], col, sem.at[p, PIECES]))
    for copy in copies:
        copy.start()

    def rest_copy(p, i):
        dst = (gate, up)[p]
        return pltpu.make_async_copy(
            rest.at[p, rows(i * GROUP, GROUP)], dst.at[rows(i * GROUP, GROUP), pl.ds(DONE, W)], rest_sem.at[p, i]
        )

    def group(i, _):
        for p in range(2):
            whole = merged_weights(raw, high, low, gainb, p, i * GROUP, NCB - 1, GROUP) * part[p, NCB - 1, :1]
            rest[p, rows(i * GROUP, GROUP), :] = whole.astype(BF16)
        for p in range(2):
            rest_copy(p, i).start()
        return 0

    lax.fori_loop(0, N // GROUP, group, 0)
    for copy in copies:
        copy.wait()
    for i in range(N // GROUP):
        for p in range(2):
            rest_copy(p, i).wait()


def per_device(train_gate, low_gate, high_gate, train_up, low_up, high_up, norm_gain):
    anywhere = pl.BlockSpec(memory_space=pltpu.HBM)
    vmem = pl.BlockSpec(memory_space=pltpu.VMEM)
    dma = pltpu.SemaphoreType.DMA
    kept = pl.pallas_call(
        gather,
        name="gather",
        out_shape=(
            pltpu.VMEM((2, N * ROWS, DONE), BF16),
            pltpu.VMEM((2, 1, COLS), F32),
            pltpu.VMEM((2, N, NCB, ROWS, W), BF16),
            pltpu.VMEM((2, RANK, COLS), BF16),
            pltpu.VMEM((2, N * ROWS, RANK), BF16),
            pltpu.VMEM((N * ROWS, ROWS), F32),
            pltpu.VMEM((2, NCB, 8, W), F32),
        ),
        in_specs=[anywhere] * 7,
        out_specs=(vmem,) * 7,
        scratch_shapes=[
            pltpu.VMEM((N, 2 * RANK, ROWS), BF16),
            pltpu.VMEM((N, 1, ROWS), F32),
            dma((2, NCB)),
            dma((5,)),
            dma((2, SIDE + 8)),
            dma((2,)),
            dma((2, 8)),
            dma((2, SIDE + 8)),
            dma,
            dma((2 * NCB + 2,)),
            dma((2, 9)),
        ],
        compiler_params=pltpu.CompilerParams(
            collective_id=0, has_side_effects=True, vmem_limit_bytes=8 * 2**20
        ),
    )(*(
        pltpu.with_memory_space_constraint(a, pltpu.HBM)
        for a in (train_gate, low_gate.T, high_gate, train_up, low_up.T, high_up, norm_gain.reshape(1, ROWS))
    ))
    hbm = pl.BlockSpec(memory_space=pltpu.HBM)
    gate, up, col_gate, col_up = pl.pallas_call(
        write,
        name="write",
        out_shape=(
            jax.ShapeDtypeStruct((N * ROWS, COLS), BF16),
            jax.ShapeDtypeStruct((N * ROWS, COLS), BF16),
            jax.ShapeDtypeStruct((1, COLS), F32),
            jax.ShapeDtypeStruct((1, COLS), F32),
        ),
        in_specs=[vmem] * 7,
        out_specs=(hbm,) * 4,
        scratch_shapes=[pltpu.VMEM((2, N * ROWS, W), BF16), dma((2, PIECES + 1)), dma((2, N // GROUP))],
        compiler_params=pltpu.CompilerParams(vmem_limit_bytes=12 * 2**20),
    )(*kept)
    return gate, up, col_gate.reshape(COLS), col_up.reshape(COLS)


def solution(mesh):
    placed = (
        P(("trial", "fsdp"), "cols"),
        P(("trial", "fsdp"), None),
        P("trial", "cols"),
        P(("trial", "fsdp"), "cols"),
        P(("trial", "fsdp"), None),
        P("trial", "cols"),
        P(("trial", "fsdp")),
    )
    return jax.shard_map(
        per_device,
        mesh=mesh,
        in_specs=placed,
        out_specs=(
            P("trial", "cols"),
            P("trial", "cols"),
            P(("trial", "cols")),
            P(("trial", "cols")),
        ),
        check_vma=False,
    )
```

```python
import functools

import jax
import jax.numpy as jnp
from jax import lax
from jax.experimental import pallas as pl
from jax.experimental.pallas import tpu as pltpu
from jax.sharding import PartitionSpec as P

MESH = pl.DeviceIdType.MESH
BF16, F32 = jnp.bfloat16, jnp.float32

N = 16
ROWS = 128
COLS = 2048
RANK = 16
NCB = 4
W = COLS // NCB
GROUP = 2
LEFT = 2
DONE = (NCB - LEFT) * W
SIDE = 28


def rows(src, n=1):
    return pl.ds(pl.multiple_of(src * ROWS, ROWS), n * ROWS)


def columns(cb):
    return pl.ds(pl.multiple_of(cb * W, W), W)


def merged_weights(raw, high, low, gainb, p, src, cb, n):
    train = raw[p, pl.ds(src, n), cb].reshape(n * ROWS, W).astype(F32)
    delta = jnp.dot(low[p, rows(src, n), :], high[p, :, columns(cb)], preferred_element_type=F32)
    scale = gainb[rows(src, n), :]
    return (train + delta) * jnp.concatenate([scale] * (W // ROWS), axis=1)


def gather(
    tg, lg, hg, tu, lu, hu, gn,
    out, cmax, raw, high, low, gainb, part,
    side, gain,
    load_sem, side_sem, ring_recv, ring_send, side_send, pair_recv, pair_send, own_recv, own_send,
):
    trial, me, cols = lax.axis_index("trial"), lax.axis_index("fsdp"), lax.axis_index("cols")
    right, left = lax.rem(me + 2, N), lax.rem(me + N - 2, N)
    pair = me + 1 - 2 * lax.rem(me, 2)
    ahead = (right, left)

    def to(f):
        return (trial, f, cols)

    def source(f, way, hops):
        return lax.rem(f + N - 2 * hops, N) if way == 0 else lax.rem(f + 2 * hops, N)

    loads = []
    for p, (low_in, high_in) in enumerate(((lg, hg), (lu, hu))):
        loads.append(pltpu.make_async_copy(low_in, side.at[me, pl.ds(p * RANK, RANK)], side_sem.at[p]))
        loads.append(pltpu.make_async_copy(high_in, high.at[p], side_sem.at[2 + p]))
    loads.append(pltpu.make_async_copy(gn, gain.at[me], side_sem.at[4]))

    def own_load(p, cb):
        train = (tg, tu)[p]
        return pltpu.make_async_copy(
            train.at[:, pl.ds(pl.multiple_of(cb * W, W), W)], raw.at[p, me, cb], load_sem.at[p, cb]
        )

    for copy in loads:
        copy.start()
    for cb in range(NCB):
        for p in range(2):
            own_load(p, cb).start()

    barrier = pltpu.get_barrier_semaphore()
    for f in (right, left, pair):
        pl.semaphore_signal(barrier, inc=1, device_id=to(f), device_id_type=MESH)
    pl.semaphore_wait(barrier, 3)

    def remote(ref, send, recv, f):
        return pltpu.make_async_remote_copy(
            src_ref=ref, dst_ref=ref, send_sem=send, recv_sem=recv, device_id=to(f), device_id_type=MESH
        )

    def chunk_at(hops, cb, short):
        return (hops - 1) * 2 * NCB + cb * 2 + short

    def ring_chunk(way, p, src, cb, at):
        return remote(raw.at[p, src, cb], ring_send.at[way], ring_recv.at[way, at], ahead[way])

    def pair_chunk(way, p, src, cb, at):
        return remote(raw.at[p, src, cb], pair_send, pair_recv.at[way, at], pair)

    def own_chunk(p, src, cb):
        return remote(raw.at[p, src, cb], pair_send, own_recv.at[p * NCB + cb], pair)

    def side_ref(way, src, hops):
        return side.at[src, pl.ds(way * RANK, RANK)] if hops == 4 else side.at[src]

    def ring_side(way, src, hops):
        copies = [remote(side_ref(way, src, hops), side_send.at[way, hops - 1], ring_recv.at[way, SIDE + hops - 1], ahead[way])]
        if way == 0 or hops < 4:
            copies.append(remote(gain.at[src], side_send.at[way, 3 + hops], ring_recv.at[way, SIDE + 3 + hops], ahead[way]))
        return copies

    def pair_side(way, src, hops):
        copies = [remote(side_ref(way, src, hops), own_send.at[way, hops - 1], pair_recv.at[way, SIDE + hops - 1], pair)]
        if way == 0 or hops < 4:
            copies.append(remote(gain.at[src], own_send.at[way, 3 + hops], pair_recv.at[way, SIDE + 3 + hops], pair))
        return copies

    def own_side(src):
        return [
            remote(side.at[src], own_send.at[0, 8], own_recv.at[2 * NCB], pair),
            remote(gain.at[src], own_send.at[1, 8], own_recv.at[2 * NCB + 1], pair),
        ]

    for copy in loads:
        copy.wait()
    for way in range(2):
        for copy in ring_side(way, me, 1):
            copy.start()
    for copy in own_side(me):
        copy.start()

    def send_own(cb, _):
        for p in range(2):
            own_load(p, cb).wait()
        for k in range(2):
            for way in range(2):
                p = way if k == 0 else 1 - way
                ring_chunk(way, p, me, cb, chunk_at(1, cb, k)).start()
        for p in range(2):
            own_chunk(p, me, cb).start()
        return 0

    lax.fori_loop(0, NCB, send_own, 0)

    def prepare(src):
        for p in range(2):
            low[p, rows(src), :] = side[src, pl.ds(p * RANK, RANK), :].astype(F32).T.astype(BF16)
        gainb[rows(src), :] = jnp.broadcast_to(gain[src], (ROWS, ROWS)).T

    merged = functools.partial(merged_weights, raw, high, low, gainb)

    def note(p, src, cb):
        size = jnp.abs(merged(p, src, cb, 1)).reshape(ROWS // 8, 8, W).max(axis=0)
        part[p, cb] = jnp.maximum(part[p, cb], size)

    part[...] = jnp.zeros_like(part)
    prepare(me)

    def note_own(cb, _):
        for p in range(2):
            note(p, me, cb)
        return 0

    lax.fori_loop(0, NCB, note_own, 0)

    for copy in own_side(pair):
        copy.wait_recv()
    prepare(pair)

    def note_pair(cb, _):
        for p in range(2):
            own_chunk(p, pair, cb).wait_recv()
            note(p, pair, cb)
        return 0

    lax.fori_loop(0, NCB, note_pair, 0)

    def pieces(f, hops):
        for k in range(2 if hops < 4 else 1):
            for way in range(2):
                yield way, (way if k == 0 else 1 - way), source(f, way, hops), k

    def at_hop(hops, cb, k):
        return chunk_at(hops, cb, k) if hops < 4 else 6 * NCB + cb

    def forward(hops, cb, ks=(0, 1)):
        for way, p, src, k in pieces(me, hops):
            if k in ks:
                ring_chunk(way, p, src, cb, at_hop(hops + 1, cb, k)).start()

    def receive(hops, cb, ks=(), relay=True):
        for way, p, src, k in pieces(me, hops):
            ring_chunk(way, p, src, cb, at_hop(hops, cb, k)).wait_recv()
            if k in ks:
                ring_chunk(way, p, src, cb, at_hop(hops + 1, cb, k)).start()
            pair_chunk(way, p, src, cb, at_hop(hops, cb, k)).start()

    def note_own_side(hops, cb):
        for way, p, src, k in pieces(me, hops):
            note(p, src, cb)

    def note_other_core(hops, cb):
        for way, p, src, k in pieces(pair, hops):
            pair_chunk(way, p, src, cb, at_hop(hops, cb, k)).wait_recv()
            note(p, src, cb)

    def sides(hops):
        for way in range(2):
            src = source(me, way, hops)
            for copy in ring_side(way, src, hops):
                copy.wait_recv()
            for copy in (ring_side(way, src, hops + 1) if hops < 4 else []) + pair_side(way, src, hops):
                copy.start()
            if hops < 4 or way == 1:
                prepare(src)
        for way in range(2):
            src = source(pair, way, hops)
            for copy in pair_side(way, src, hops):
                copy.wait_recv()
            if hops < 4 or way == 1:
                prepare(src)

    def settle(cb):
        for p in range(2):
            largest = part[p, cb].max(axis=0, keepdims=True)
            cmax[p, :, columns(cb)] = largest
            part[p, cb] = jnp.broadcast_to(1.0 / largest, (8, W))

    def scale(cb):
        def group(i, _):
            for p in range(2):
                whole = merged(p, i * GROUP, cb, GROUP) * part[p, cb, :1]
                out[p, rows(i * GROUP, GROUP), columns(cb)] = whole.astype(BF16)
            return 0

        lax.fori_loop(0, N // GROUP, group, 0)

    sides(1)

    def step(cb, _):
        receive(1, cb, (0, 1))
        note_own_side(1, cb)
        note_other_core(1, cb)
        return 0

    lax.fori_loop(0, NCB, step, 0)

    sides(2)

    def step_2(cb, _):
        receive(2, cb)

        @pl.when(cb < 2)
        def _():
            forward(2, cb)

        note_own_side(2, cb)
        note_other_core(2, cb)
        return 0

    lax.fori_loop(0, NCB, step_2, 0)
    sides(3)
    for hops, cb in ((3, 0), (3, 1), (4, 0), (4, 1), (3, 2), (3, 3), (4, 2), (4, 3)):
        if hops == 4 and cb == 0:
            sides(4)
        receive(hops, cb, (0,) if hops == 3 else ())
        if hops == 3 and cb == 1:
            forward(2, 2)
            forward(2, 3)
        note_own_side(hops, cb)
        if hops == 4:
            if cb % 2 == 0:
                note_other_core(3, cb)
                note_other_core(3, cb + 1)
            note_other_core(4, cb)
            settle(cb)
            if cb < NCB - LEFT:
                scale(cb)

    for way in range(2):
        sent = raw.at[0, pl.ds(0, 7)]
        pltpu.make_async_copy(sent, sent, ring_send.at[way]).wait()
        for hops in (1, 2, 3, 4):
            src = source(me, way, hops - 1)
            for copy in ring_side(way, src, hops):
                copy.wait_send()
            for copy in pair_side(way, source(me, way, hops), hops):
                copy.wait_send()
    for copy in own_side(me):
        copy.wait_send()
    pltpu.make_async_copy(raw.at[0], raw.at[0], pair_send).wait()


PIECES = 8


def write(new, cmax, raw, high, low, gainb, part, gate, up, col_gate, col_up, rest, sem, rest_sem):
    copies = []
    for i in range(PIECES):
        at = pl.ds(i * (N * ROWS // PIECES), N * ROWS // PIECES)
        for p, dst in enumerate((gate, up)):
            copies.append(pltpu.make_async_copy(new.at[p, at], dst.at[at, pl.ds(0, DONE)], sem.at[p, i]))
    for p, col in enumerate((col_gate, col_up)):
        copies.append(pltpu.make_async_copy(cmax.at[p], col, sem.at[p, PIECES]))
    for copy in copies:
        copy.start()

    def rest_copy(p, cb, i):
        dst = (gate, up)[p]
        return pltpu.make_async_copy(
            rest.at[p, cb, rows(i * GROUP, GROUP)],
            dst.at[rows(i * GROUP, GROUP), pl.ds(pl.multiple_of(DONE + cb * W, W), W)],
            rest_sem.at[p, cb, i],
        )

    def group(j, _):
        cb, i = j // (N // GROUP), lax.rem(j, N // GROUP)
        for p in range(2):
            whole = merged_weights(raw, high, low, gainb, p, i * GROUP, NCB - LEFT + cb, GROUP)
            rest[p, cb, rows(i * GROUP, GROUP), :] = (whole * part[p, NCB - LEFT + cb, :1]).astype(BF16)
        for p in range(2):
            rest_copy(p, cb, i).start()
        return 0

    lax.fori_loop(0, LEFT * (N // GROUP), group, 0)
    for copy in copies:
        copy.wait()
    for cb in range(LEFT):
        for i in range(N // GROUP):
            for p in range(2):
                rest_copy(p, cb, i).wait()


def per_device(train_gate, low_gate, high_gate, train_up, low_up, high_up, norm_gain):
    anywhere = pl.BlockSpec(memory_space=pltpu.HBM)
    vmem = pl.BlockSpec(memory_space=pltpu.VMEM)
    dma = pltpu.SemaphoreType.DMA
    kept = pl.pallas_call(
        gather,
        name="gather",
        out_shape=(
            pltpu.VMEM((2, N * ROWS, DONE), BF16),
            pltpu.VMEM((2, 1, COLS), F32),
            pltpu.VMEM((2, N, NCB, ROWS, W), BF16),
            pltpu.VMEM((2, RANK, COLS), BF16),
            pltpu.VMEM((2, N * ROWS, RANK), BF16),
            pltpu.VMEM((N * ROWS, ROWS), F32),
            pltpu.VMEM((2, NCB, 8, W), F32),
        ),
        in_specs=[anywhere] * 7,
        out_specs=(vmem,) * 7,
        scratch_shapes=[
            pltpu.VMEM((N, 2 * RANK, ROWS), BF16),
            pltpu.VMEM((N, 1, ROWS), F32),
            dma((2, NCB)),
            dma((5,)),
            dma((2, SIDE + 8)),
            dma((2,)),
            dma((2, 8)),
            dma((2, SIDE + 8)),
            dma,
            dma((2 * NCB + 2,)),
            dma((2, 9)),
        ],
        compiler_params=pltpu.CompilerParams(
            collective_id=0, has_side_effects=True, vmem_limit_bytes=8 * 2**20
        ),
    )(*(
        pltpu.with_memory_space_constraint(a, pltpu.HBM)
        for a in (train_gate, low_gate.T, high_gate, train_up, low_up.T, high_up, norm_gain.reshape(1, ROWS))
    ))
    hbm = pl.BlockSpec(memory_space=pltpu.HBM)
    gate, up, col_gate, col_up = pl.pallas_call(
        write,
        name="write",
        out_shape=(
            jax.ShapeDtypeStruct((N * ROWS, COLS), BF16),
            jax.ShapeDtypeStruct((N * ROWS, COLS), BF16),
            jax.ShapeDtypeStruct((1, COLS), F32),
            jax.ShapeDtypeStruct((1, COLS), F32),
        ),
        in_specs=[vmem] * 7,
        out_specs=(hbm,) * 4,
        scratch_shapes=[pltpu.VMEM((2, LEFT, N * ROWS, W), BF16), dma((2, PIECES + 1)), dma((2, LEFT, N // GROUP))],
        compiler_params=pltpu.CompilerParams(vmem_limit_bytes=12 * 2**20),
    )(*kept)
    return gate, up, col_gate.reshape(COLS), col_up.reshape(COLS)


def solution(mesh):
    placed = (
        P(("trial", "fsdp"), "cols"),
        P(("trial", "fsdp"), None),
        P("trial", "cols"),
        P(("trial", "fsdp"), "cols"),
        P(("trial", "fsdp"), None),
        P("trial", "cols"),
        P(("trial", "fsdp")),
    )
    return jax.shard_map(
        per_device,
        mesh=mesh,
        in_specs=placed,
        out_specs=(
            P("trial", "cols"),
            P("trial", "cols"),
            P(("trial", "cols")),
            P(("trial", "cols")),
        ),
        check_vma=False,
    )
```

```python
import functools

import jax
import jax.numpy as jnp
from jax import lax
from jax.experimental import pallas as pl
from jax.experimental.pallas import tpu as pltpu
from jax.sharding import PartitionSpec as P

MESH = pl.DeviceIdType.MESH
BF16, F32 = jnp.bfloat16, jnp.float32

N = 16
ROWS = 128
COLS = 2048
RANK = 16
NCB = 4
W = COLS // NCB
GROUP = 2
LEFT = 2
DONE = (NCB - LEFT) * W
MOVED = 1
SIDE = 28


def rows(src, n=1):
    return pl.ds(pl.multiple_of(src * ROWS, ROWS), n * ROWS)


def columns(cb):
    return pl.ds(pl.multiple_of(cb * W, W), W)


def merged_weights(raw, high, low, gainb, p, src, cb, n):
    train = raw[p, pl.ds(src, n), cb].reshape(n * ROWS, W).astype(F32)
    delta = jnp.dot(low[p, rows(src, n), :], high[p, :, columns(cb)], preferred_element_type=F32)
    scale = gainb[rows(src, n), :]
    return (train + delta) * jnp.concatenate([scale] * (W // ROWS), axis=1)


def gather(
    tg, lg, hg, tu, lu, hu, gn,
    out, cmax, raw, high, low, gainb, part,
    side, gain,
    load_sem, side_sem, ring_recv, ring_send, side_send, pair_recv, pair_send, own_recv, own_send, go, moved_send,
):
    trial, me, cols = lax.axis_index("trial"), lax.axis_index("fsdp"), lax.axis_index("cols")
    right, left = lax.rem(me + 2, N), lax.rem(me + N - 2, N)
    pair = me + 1 - 2 * lax.rem(me, 2)
    ahead = (right, left)

    def to(f):
        return (trial, f, cols)

    def source(f, way, hops):
        return lax.rem(f + N - 2 * hops, N) if way == 0 else lax.rem(f + 2 * hops, N)

    loads = []
    for p, (low_in, high_in) in enumerate(((lg, hg), (lu, hu))):
        loads.append(pltpu.make_async_copy(low_in, side.at[me, pl.ds(p * RANK, RANK)], side_sem.at[p]))
        loads.append(pltpu.make_async_copy(high_in, high.at[p], side_sem.at[2 + p]))
    loads.append(pltpu.make_async_copy(gn, gain.at[me], side_sem.at[4]))

    def own_load(p, cb):
        train = (tg, tu)[p]
        return pltpu.make_async_copy(
            train.at[:, pl.ds(pl.multiple_of(cb * W, W), W)], raw.at[p, me, cb], load_sem.at[p, cb]
        )

    for copy in loads:
        copy.start()
    for cb in range(NCB):
        for p in range(2):
            own_load(p, cb).start()

    z = me // 2
    first_right, first_left = z <= 5, (z == 0) | (z == 7)
    upward_last = (z >= 1) & (z <= 5)

    barrier = pltpu.get_barrier_semaphore()
    pl.semaphore_signal(barrier, inc=1, device_id=to(pair), device_id_type=MESH)
    for first, f in ((first_right, right), (first_left, left)):

        @pl.when(first)
        def _(f=f):
            pl.semaphore_signal(barrier, inc=1, device_id=to(f), device_id_type=MESH)

    pl.semaphore_wait(barrier, 3 - first_right.astype(jnp.int32) - first_left.astype(jnp.int32))
    for way, (first, f) in enumerate(((first_right, right), (first_left, left))):

        @pl.when(jnp.logical_not(first))
        def _(way=way, f=f):
            pl.semaphore_signal(go.at[1 - way], inc=1, device_id=to(f), device_id_type=MESH)

    def remote(ref, send, recv, f):
        return pltpu.make_async_remote_copy(
            src_ref=ref, dst_ref=ref, send_sem=send, recv_sem=recv, device_id=to(f), device_id_type=MESH
        )

    def chunk_at(hops, cb, short):
        return (hops - 1) * 2 * NCB + cb * 2 + short

    def ring_chunk(way, p, src, cb, at):
        return remote(raw.at[p, src, cb], ring_send.at[way], ring_recv.at[way, at], ahead[way])

    def pair_chunk(way, p, src, cb, at):
        return remote(raw.at[p, src, cb], pair_send, pair_recv.at[way, at], pair)

    def own_chunk(p, src, cb):
        return remote(raw.at[p, src, cb], pair_send, own_recv.at[p * NCB + cb], pair)

    def side_ref(way, src, hops):
        return side.at[src, pl.ds(way * RANK, RANK)] if hops == 4 else side.at[src]

    def ring_side(way, src, hops):
        copies = [remote(side_ref(way, src, hops), side_send.at[way, hops - 1], ring_recv.at[way, SIDE + hops - 1], ahead[way])]
        if way == 0 or hops < 4:
            copies.append(remote(gain.at[src], side_send.at[way, 3 + hops], ring_recv.at[way, SIDE + 3 + hops], ahead[way]))
        return copies

    def pair_side(way, src, hops):
        copies = [remote(side_ref(way, src, hops), own_send.at[way, hops - 1], pair_recv.at[way, SIDE + hops - 1], pair)]
        if way == 0 or hops < 4:
            copies.append(remote(gain.at[src], own_send.at[way, 3 + hops], pair_recv.at[way, SIDE + 3 + hops], pair))
        return copies

    def own_side(src):
        return [
            remote(side.at[src], own_send.at[0, 8], own_recv.at[2 * NCB], pair),
            remote(gain.at[src], own_send.at[1, 8], own_recv.at[2 * NCB + 1], pair),
        ]

    for copy in loads:
        copy.wait()

    def own_way(way, opening):
        for copy in ring_side(way, me, 1) + (own_side(me) if opening else []):
            copy.start()

        def block(cb, _):
            for k in range(2):
                p = way if k == 0 else 1 - way
                if opening:
                    own_load(p, cb).wait()
                ring_chunk(way, p, me, cb, chunk_at(1, cb, k)).start()
                if opening:
                    own_chunk(p, me, cb).start()
            return 0

        lax.fori_loop(0, NCB, block, 0)

    @pl.when(upward_last)
    def _():
        own_way(1, True)
        pl.semaphore_wait(go.at[0], 1)
        own_way(0, False)

    @pl.when(jnp.logical_not(upward_last))
    def _():
        @pl.when(z == 0)
        def _():
            pl.semaphore_wait(go.at[0], 1)

        own_way(0, True)

        @pl.when(z != 6)
        def _():
            pl.semaphore_wait(go.at[1], 1)

        own_way(1, False)

    def prepare(src):
        for p in range(2):
            low[p, rows(src), :] = side[src, pl.ds(p * RANK, RANK), :].astype(F32).T.astype(BF16)
        gainb[rows(src), :] = jnp.broadcast_to(gain[src], (ROWS, ROWS)).T

    merged = functools.partial(merged_weights, raw, high, low, gainb)

    def note(p, src, cb):
        size = jnp.abs(merged(p, src, cb, 1)).reshape(ROWS // 8, 8, W).max(axis=0)
        part[p, cb] = jnp.maximum(part[p, cb], size)

    part[...] = jnp.zeros_like(part)
    prepare(me)

    def note_own(cb, _):
        for p in range(2):
            note(p, me, cb)
        return 0

    lax.fori_loop(0, NCB, note_own, 0)

    for copy in own_side(pair):
        copy.wait_recv()
    prepare(pair)

    def note_pair(cb, _):
        for p in range(2):
            own_chunk(p, pair, cb).wait_recv()
            note(p, pair, cb)
        return 0

    lax.fori_loop(0, NCB, note_pair, 0)

    def pieces(f, hops):
        for k in range(2 if hops < 4 else 1):
            for way in range(2):
                yield way, (way if k == 0 else 1 - way), source(f, way, hops), k

    def at_hop(hops, cb, k):
        return chunk_at(hops, cb, k) if hops < 4 else 6 * NCB + cb

    def forward(hops, cb, ks=(0, 1)):
        for way, p, src, k in pieces(me, hops):
            if k in ks:
                ring_chunk(way, p, src, cb, at_hop(hops + 1, cb, k)).start()

    def moved_chunk(src, cb):
        return remote(raw.at[0, src, cb], moved_send.at[cb], ring_recv.at[1, SIDE + 8 + cb], left)

    def receive(hops, cb, ks=()):
        for way, p, src, k in pieces(me, hops):
            chunk = ring_chunk(way, p, src, cb, at_hop(hops, cb, k))
            if hops < 3 or cb < NCB - MOVED or p == 1:
                chunk.wait_recv()
                if k in ks:
                    ring_chunk(way, p, src, cb, at_hop(hops + 1, cb, k)).start()
            elif hops == 3:
                chunk.wait_recv()
                if way == 0:

                    @pl.when(z != 7)
                    def _(p=p, src=src):
                        ring_chunk(0, p, src, cb, at_hop(4, cb, 0)).start()
                else:

                    @pl.when(z == 1)
                    def _(src=src):
                        moved_chunk(src, cb).start()
            else:

                @pl.when(z == 0)
                def _(src=src):
                    moved_chunk(src, cb).wait_recv()

                @pl.when(z != 0)
                def _(chunk=chunk):
                    chunk.wait_recv()

            pair_chunk(way, p, src, cb, at_hop(hops, cb, k)).start()

    def note_own_side(hops, cb):
        for way, p, src, k in pieces(me, hops):
            note(p, src, cb)

    def note_other_core(hops, cb):
        for way, p, src, k in pieces(pair, hops):
            pair_chunk(way, p, src, cb, at_hop(hops, cb, k)).wait_recv()
            note(p, src, cb)

    def sides(hops):
        for way in range(2):
            src = source(me, way, hops)
            for copy in ring_side(way, src, hops):
                copy.wait_recv()
            for copy in (ring_side(way, src, hops + 1) if hops < 4 else []) + pair_side(way, src, hops):
                copy.start()
            if hops < 4 or way == 1:
                prepare(src)
        for way in range(2):
            src = source(pair, way, hops)
            for copy in pair_side(way, src, hops):
                copy.wait_recv()
            if hops < 4 or way == 1:
                prepare(src)

    def settle(cb):
        for p in range(2):
            largest = part[p, cb].max(axis=0, keepdims=True)
            cmax[p, :, columns(cb)] = largest
            part[p, cb] = jnp.broadcast_to(1.0 / largest, (8, W))

    def scale(cb):
        def group(i, _):
            for p in range(2):
                whole = merged(p, i * GROUP, cb, GROUP) * part[p, cb, :1]
                out[p, rows(i * GROUP, GROUP), columns(cb)] = whole.astype(BF16)
            return 0

        lax.fori_loop(0, N // GROUP, group, 0)

    sides(1)

    def step(cb, _):
        receive(1, cb, (0, 1))
        note_own_side(1, cb)
        note_other_core(1, cb)
        return 0

    lax.fori_loop(0, NCB, step, 0)

    sides(2)

    def step_2(cb, _):
        receive(2, cb)

        @pl.when(cb < 2)
        def _():
            forward(2, cb)

        note_own_side(2, cb)
        note_other_core(2, cb)
        return 0

    lax.fori_loop(0, NCB, step_2, 0)
    sides(3)
    for hops, cb in ((3, 0), (3, 1), (4, 0), (4, 1), (3, 2), (3, 3), (4, 2), (4, 3)):
        if hops == 4 and cb == 0:
            sides(4)
        receive(hops, cb, (0,) if hops == 3 else ())
        if hops == 3 and cb == 1:
            forward(2, 2)
            forward(2, 3)
        note_own_side(hops, cb)
        if hops == 4:
            if cb % 2 == 0:
                note_other_core(3, cb)
                note_other_core(3, cb + 1)
            note_other_core(4, cb)
            settle(cb)
            if cb < NCB - LEFT:
                scale(cb)

    for way in range(2):
        sent = raw.at[0, pl.ds(0, 7)]
        if way == 0:
            fewer = raw.at[0, pl.ds(0, 9), pl.ds(0, 3)] if MOVED == 1 else raw.at[0, pl.ds(0, 13), pl.ds(0, 2)]

            @pl.when(z == 7)
            def _(fewer=fewer):
                pltpu.make_async_copy(fewer, fewer, ring_send.at[0]).wait()

            @pl.when(z != 7)
            def _(sent=sent):
                pltpu.make_async_copy(sent, sent, ring_send.at[0]).wait()
        else:
            pltpu.make_async_copy(sent, sent, ring_send.at[1]).wait()

            @pl.when(z == 1)
            def _():
                for cb in range(NCB - MOVED, NCB):
                    moved_chunk(source(me, 1, 3), cb).wait_send()
        for hops in (1, 2, 3, 4):
            src = source(me, way, hops - 1)
            for copy in ring_side(way, src, hops):
                copy.wait_send()
            for copy in pair_side(way, source(me, way, hops), hops):
                copy.wait_send()
    for copy in own_side(me):
        copy.wait_send()
    pltpu.make_async_copy(raw.at[0], raw.at[0], pair_send).wait()


PIECES = 8


def write(new, cmax, raw, high, low, gainb, part, gate, up, col_gate, col_up, rest, sem, rest_sem):
    copies = []
    for i in range(PIECES):
        at = pl.ds(i * (N * ROWS // PIECES), N * ROWS // PIECES)
        for p, dst in enumerate((gate, up)):
            copies.append(pltpu.make_async_copy(new.at[p, at], dst.at[at, pl.ds(0, DONE)], sem.at[p, i]))
    for p, col in enumerate((col_gate, col_up)):
        copies.append(pltpu.make_async_copy(cmax.at[p], col, sem.at[p, PIECES]))
    for copy in copies:
        copy.start()

    def rest_copy(p, cb, i):
        dst = (gate, up)[p]
        return pltpu.make_async_copy(
            rest.at[p, cb, rows(i * GROUP, GROUP)],
            dst.at[rows(i * GROUP, GROUP), pl.ds(pl.multiple_of(DONE + cb * W, W), W)],
            rest_sem.at[p, cb, i],
        )

    def group(j, _):
        cb, i = j // (N // GROUP), lax.rem(j, N // GROUP)
        for p in range(2):
            whole = merged_weights(raw, high, low, gainb, p, i * GROUP, NCB - LEFT + cb, GROUP)
            rest[p, cb, rows(i * GROUP, GROUP), :] = (whole * part[p, NCB - LEFT + cb, :1]).astype(BF16)
        for p in range(2):
            rest_copy(p, cb, i).start()
        return 0

    lax.fori_loop(0, LEFT * (N // GROUP), group, 0)
    for copy in copies:
        copy.wait()
    for cb in range(LEFT):
        for i in range(N // GROUP):
            for p in range(2):
                rest_copy(p, cb, i).wait()


def per_device(train_gate, low_gate, high_gate, train_up, low_up, high_up, norm_gain):
    anywhere = pl.BlockSpec(memory_space=pltpu.HBM)
    vmem = pl.BlockSpec(memory_space=pltpu.VMEM)
    dma = pltpu.SemaphoreType.DMA
    kept = pl.pallas_call(
        gather,
        name="gather",
        out_shape=(
            pltpu.VMEM((2, N * ROWS, DONE), BF16),
            pltpu.VMEM((2, 1, COLS), F32),
            pltpu.VMEM((2, N, NCB, ROWS, W), BF16),
            pltpu.VMEM((2, RANK, COLS), BF16),
            pltpu.VMEM((2, N * ROWS, RANK), BF16),
            pltpu.VMEM((N * ROWS, ROWS), F32),
            pltpu.VMEM((2, NCB, 8, W), F32),
        ),
        in_specs=[anywhere] * 7,
        out_specs=(vmem,) * 7,
        scratch_shapes=[
            pltpu.VMEM((N, 2 * RANK, ROWS), BF16),
            pltpu.VMEM((N, 1, ROWS), F32),
            dma((2, NCB)),
            dma((5,)),
            dma((2, SIDE + 8 + NCB)),
            dma((2,)),
            dma((2, 8)),
            dma((2, SIDE + 8)),
            dma,
            dma((2 * NCB + 2,)),
            dma((2, 9)),
            pltpu.SemaphoreType.REGULAR((2,)),
            dma((NCB,)),
        ],
        compiler_params=pltpu.CompilerParams(
            collective_id=0, has_side_effects=True, vmem_limit_bytes=8 * 2**20
        ),
    )(*(
        pltpu.with_memory_space_constraint(a, pltpu.HBM)
        for a in (train_gate, low_gate.T, high_gate, train_up, low_up.T, high_up, norm_gain.reshape(1, ROWS))
    ))
    hbm = pl.BlockSpec(memory_space=pltpu.HBM)
    gate, up, col_gate, col_up = pl.pallas_call(
        write,
        name="write",
        out_shape=(
            jax.ShapeDtypeStruct((N * ROWS, COLS), BF16),
            jax.ShapeDtypeStruct((N * ROWS, COLS), BF16),
            jax.ShapeDtypeStruct((1, COLS), F32),
            jax.ShapeDtypeStruct((1, COLS), F32),
        ),
        in_specs=[vmem] * 7,
        out_specs=(hbm,) * 4,
        scratch_shapes=[pltpu.VMEM((2, LEFT, N * ROWS, W), BF16), dma((2, PIECES + 1)), dma((2, LEFT, N // GROUP))],
        compiler_params=pltpu.CompilerParams(vmem_limit_bytes=12 * 2**20),
    )(*kept)
    return gate, up, col_gate.reshape(COLS), col_up.reshape(COLS)


def solution(mesh):
    placed = (
        P(("trial", "fsdp"), "cols"),
        P(("trial", "fsdp"), None),
        P("trial", "cols"),
        P(("trial", "fsdp"), "cols"),
        P(("trial", "fsdp"), None),
        P("trial", "cols"),
        P(("trial", "fsdp")),
    )
    return jax.shard_map(
        per_device,
        mesh=mesh,
        in_specs=placed,
        out_specs=(
            P("trial", "cols"),
            P("trial", "cols"),
            P(("trial", "cols")),
            P(("trial", "cols")),
        ),
        check_vma=False,
    )
```
